16 devices in a mesh: tp: 4 (over z, y), ep: 4 (over x, core).
Axes of the slice: x: 2, y: 2, z: 2, core: 2. Of those that a mesh axis runs over, the one named last changes fastest.
Arguments:
- x_tok: bfloat16 [32768, 512], P('ep')
- dy_tok: bfloat16 [32768, 512], P('ep')
- route_idx: int32 [32768, 2], P('ep')
- norm_scale: float32 [512], replicated
- w_router: float32 [512, 32], replicated
- w_gate: bfloat16 [32, 512, 2048], P('ep', None, 'tp')
- w_lin: bfloat16 [32, 512, 2048], P('ep', None, 'tp')
- w_out: bfloat16 [32, 2048, 512], P('ep', 'tp')
Outputs:
- output 1: bfloat16 [32768, 512], P('ep')
- output 2: float32 [2], replicated
- output 3: bfloat16 [32768, 512], P('ep')
- output 4: float32 [512], replicated
- output 5: float32 [512, 32], replicated
- output 6: float32 [32, 512, 2048], P('ep', None, 'tp')
- output 7: float32 [32, 512, 2048], P('ep', None, 'tp')
- output 8: float32 [32, 2048, 512], P('ep', 'tp')
All inputs are finite; a program needn't handle non-finite values.
Results may differ from the reference program's by a relative error of at most 0.0165257.
Values are sent between devices in bfloat16 or wider.
A program may use at most 1 GiB of HBM per device.

```python
import jax
import jax.numpy as jnp
from jax import lax

MODEL_DIM = 512
FF_DIM = 2048
EXPERTS = 32
TOK_DEV = 8192
GROUPS = 4
TOKENS = TOK_DEV * GROUPS
SLOT_CAP = (5 * TOK_DEV + 2 * EXPERTS - 1) // (2 * EXPERTS)
NORM_EPS = 1e-6
Z_COEF = 0.001
AUX_COEF = 0.01


def draw_routes(root_key, tok_count, expert_count):
    sub_keys = jax.random.split(root_key, 4)
    expert_order = jax.random.permutation(sub_keys[0], expert_count)
    pick_left = jax.random.randint(sub_keys[1], (tok_count,), 0, expert_count)
    pick_right = jax.random.randint(sub_keys[2], (tok_count,), 0, expert_count)
    first_ids = expert_order[jnp.minimum(pick_left, pick_right)]
    step_size = jax.random.randint(sub_keys[3], (tok_count,), 1, expert_count)
    second_ids = (first_ids + step_size) % expert_count
    return jnp.stack([first_ids, second_ids], axis=1).astype(jnp.int32)


def setup_inputs(seed: int = 0) -> dict:
    sub_keys = jax.random.split(jax.random.key(seed), 8)
    x_tok = jax.random.normal(sub_keys[0], (TOKENS, MODEL_DIM), jnp.float32).astype(jnp.bfloat16)
    dy_tok = (jax.random.normal(sub_keys[1], (TOKENS, MODEL_DIM), jnp.float32) * MODEL_DIM ** -0.5).astype(jnp.bfloat16)
    route_idx = draw_routes(sub_keys[2], TOKENS, EXPERTS)
    norm_scale = 1.0 + 0.3 * jax.random.normal(sub_keys[3], (MODEL_DIM,), jnp.float32)
    w_router = jax.random.normal(sub_keys[4], (MODEL_DIM, EXPERTS), jnp.float32) * (4.0 * MODEL_DIM ** -0.5)
    w_gate = (jax.random.normal(sub_keys[5], (EXPERTS, MODEL_DIM, FF_DIM), jnp.float32) * MODEL_DIM ** -0.5).astype(jnp.bfloat16)
    w_lin = (jax.random.normal(sub_keys[6], (EXPERTS, MODEL_DIM, FF_DIM), jnp.float32) * MODEL_DIM ** -0.5).astype(jnp.bfloat16)
    w_out = (jax.random.normal(sub_keys[7], (EXPERTS, FF_DIM, MODEL_DIM), jnp.float32) * (1.5 * FF_DIM ** -0.5)).astype(jnp.bfloat16)
    return {'x_tok': x_tok, 'dy_tok': dy_tok, 'route_idx': route_idx, 'norm_scale': norm_scale, 'w_router': w_router, 'w_gate': w_gate, 'w_lin': w_lin, 'w_out': w_out}


def gelu_fn(pre_act):
    return jax.nn.gelu(pre_act, approximate=True)


def route_slots(route_ids, experts, slot_cap, stride):
    expert_ids = jnp.arange(experts, dtype=jnp.int32)
    hit_first = (route_ids[:, 0:1] == expert_ids).astype(jnp.int32)
    hit_second = (route_ids[:, 1:2] == expert_ids).astype(jnp.int32)
    rank_first = jnp.cumsum(hit_first, axis=0) - hit_first
    rank_second = jnp.cumsum(hit_second, axis=0) - hit_second + jnp.sum(hit_first, axis=0)
    pos_first = jnp.sum(rank_first * hit_first, axis=1)
    pos_second = jnp.sum(rank_second * hit_second, axis=1)
    overflow = experts * stride
    slot_first = jnp.where(pos_first < slot_cap, route_ids[:, 0] * stride + pos_first, overflow)
    slot_second = jnp.where(pos_second < slot_cap, route_ids[:, 1] * stride + pos_second, overflow)
    return slot_first, slot_second


def slot_tables(slot_first, slot_second, gate_first, gate_second, slot_total):
    tok_count = slot_first.shape[0]
    tok_ids = jnp.arange(tok_count, dtype=jnp.int32)
    slot_tok = jnp.full((slot_total + 1,), tok_count, jnp.int32)
    slot_tok = slot_tok.at[slot_first].set(tok_ids).at[slot_second].set(tok_ids)
    slot_gate = jnp.zeros((slot_total + 1,), jnp.float32)
    slot_gate = slot_gate.at[slot_first].set(gate_first).at[slot_second].set(gate_second)
    return slot_tok[:slot_total], slot_gate[:slot_total]


def pick_rows(row_data, slot_index):
    return jnp.take(row_data, slot_index, axis=0, mode='fill', fill_value=0)


def reference(x_tok, dy_tok, route_idx, norm_scale, w_router, w_gate, w_lin, w_out):
    x_wide = x_tok.astype(jnp.float32)
    inv_rms = lax.rsqrt(jnp.mean(x_wide * x_wide, axis=-1, keepdims=True) + NORM_EPS)
    x_norm = x_wide * inv_rms
    u_tok = (x_norm * norm_scale).astype(jnp.bfloat16)
    u_wide = u_tok.astype(jnp.float32)
    logits = jnp.dot(u_wide, w_router, preferred_element_type=jnp.float32)
    log_norm = jax.nn.logsumexp(logits, axis=-1)
    router_prob = jnp.exp(logits - log_norm[:, None])
    expert_ids = jnp.arange(EXPERTS, dtype=jnp.int32)
    one_first = (route_idx[:, 0:1] == expert_ids).astype(jnp.float32)
    one_second = (route_idx[:, 1:2] == expert_ids).astype(jnp.float32)
    frac_first = jnp.sum(one_first, axis=0) / TOKENS
    mean_prob = jnp.sum(router_prob, axis=0) / TOKENS
    z_loss = Z_COEF * jnp.sum(log_norm * log_norm) / TOKENS
    aux_loss = AUX_COEF * EXPERTS * jnp.sum(frac_first * mean_prob)
    gate_first = jnp.sum(router_prob * one_first, axis=-1)
    gate_second = jnp.sum(router_prob * one_second, axis=-1)
    gate_total = gate_first + gate_second
    norm_first = gate_first / gate_total
    norm_second = gate_second / gate_total
    gate_wide = w_gate.astype(jnp.float32)
    lin_wide = w_lin.astype(jnp.float32)
    out_wide = w_out.astype(jnp.float32)

    def group_step(grad_acc, group_in):
        ids_grp, u_grp, dy_grp, first_grp, second_grp = group_in
        slot_first, slot_second = route_slots(ids_grp, EXPERTS, SLOT_CAP, SLOT_CAP)
        slot_tok, slot_gate = slot_tables(slot_first, slot_second, first_grp, second_grp, EXPERTS * SLOT_CAP)
        disp_rows = pick_rows(u_grp, slot_tok).reshape(EXPERTS, SLOT_CAP, MODEL_DIM).astype(jnp.float32)
        a_gate = jnp.einsum('ecd,edf->ecf', disp_rows, gate_wide)
        a_lin = jnp.einsum('ecd,edf->ecf', disp_rows, lin_wide)
        gelu_val, gelu_back = jax.vjp(gelu_fn, a_gate)
        hidden = (gelu_val * a_lin).astype(jnp.bfloat16).astype(jnp.float32)
        exp_out = jnp.einsum('ecf,efd->ecd', hidden, out_wide).astype(jnp.bfloat16)
        exp_out = exp_out.reshape(EXPERTS * SLOT_CAP, MODEL_DIM)
        out_first = pick_rows(exp_out, slot_first)
        out_second = pick_rows(exp_out, slot_second)
        do_slot = (pick_rows(dy_grp, slot_tok).astype(jnp.float32) * slot_gate[:, None]).astype(jnp.bfloat16)
        do_slot = do_slot.astype(jnp.float32).reshape(EXPERTS, SLOT_CAP, MODEL_DIM)
        d_hidden = jnp.einsum('ecd,efd->ecf', do_slot, out_wide)
        da_gate = gelu_back(d_hidden * a_lin)[0].astype(jnp.bfloat16).astype(jnp.float32)
        da_lin = (d_hidden * gelu_val).astype(jnp.bfloat16).astype(jnp.float32)
        du_slot = jnp.einsum('ecf,edf->ecd', da_gate, gate_wide) + jnp.einsum('ecf,edf->ecd', da_lin, lin_wide)
        du_slot = du_slot.astype(jnp.bfloat16).reshape(EXPERTS * SLOT_CAP, MODEL_DIM)
        du_exp = pick_rows(du_slot, slot_first).astype(jnp.float32) + pick_rows(du_slot, slot_second).astype(jnp.float32)
        acc_gate, acc_lin, acc_out = grad_acc
        acc_gate = acc_gate + jnp.einsum('ecd,ecf->edf', disp_rows, da_gate)
        acc_lin = acc_lin + jnp.einsum('ecd,ecf->edf', disp_rows, da_lin)
        acc_out = acc_out + jnp.einsum('ecf,ecd->efd', hidden, do_slot)
        return (acc_gate, acc_lin, acc_out), (out_first, out_second, du_exp)

    group_in = (route_idx.reshape(GROUPS, TOK_DEV, 2), u_tok.reshape(GROUPS, TOK_DEV, MODEL_DIM), dy_tok.reshape(GROUPS, TOK_DEV, MODEL_DIM), norm_first.reshape(GROUPS, TOK_DEV), norm_second.reshape(GROUPS, TOK_DEV))
    grad_init = (jnp.zeros((EXPERTS, MODEL_DIM, FF_DIM), jnp.float32), jnp.zeros((EXPERTS, MODEL_DIM, FF_DIM), jnp.float32), jnp.zeros((EXPERTS, FF_DIM, MODEL_DIM), jnp.float32))
    grad_sums, per_group = lax.scan(group_step, grad_init, group_in)
    d_gate, d_lin, d_out = grad_sums
    out_first = per_group[0].reshape(TOKENS, MODEL_DIM).astype(jnp.float32)
    out_second = per_group[1].reshape(TOKENS, MODEL_DIM).astype(jnp.float32)
    du_exp = per_group[2].reshape(TOKENS, MODEL_DIM)
    y_tok = (x_wide + norm_first[:, None] * out_first + norm_second[:, None] * out_second).astype(jnp.bfloat16)
    dy_wide = dy_tok.astype(jnp.float32)
    dn_first = jnp.sum(dy_wide * out_first, axis=-1)
    dn_second = jnp.sum(dy_wide * out_second, axis=-1)
    gate_mix = norm_first * dn_first + norm_second * dn_second
    aux_coef = AUX_COEF * EXPERTS * frac_first
    d_logits = router_prob * (aux_coef - jnp.sum(aux_coef * router_prob, axis=-1, keepdims=True))
    d_logits = d_logits + (2.0 * Z_COEF) * log_norm[:, None] * router_prob
    d_logits = d_logits + one_first * (norm_first * (dn_first - gate_mix))[:, None]
    d_logits = d_logits + one_second * (norm_second * (dn_second - gate_mix))[:, None]
    d_router = jnp.dot(u_wide.T, d_logits, preferred_element_type=jnp.float32)
    du_all = du_exp + jnp.dot(d_logits, w_router.T, preferred_element_type=jnp.float32)
    d_scale = jnp.sum(du_all * x_norm, axis=0)
    dx_norm = du_all * norm_scale
    dx_tok = (dy_wide + inv_rms * (dx_norm - x_norm * jnp.mean(dx_norm * x_norm, axis=-1, keepdims=True))).astype(jnp.bfloat16)
    losses = jnp.stack([z_loss, aux_loss])
    return (y_tok, losses, dx_tok, d_scale, d_router, d_gate, d_lin, d_out)
```

```python
import functools

import jax
import jax.numpy as jnp
from jax import lax
from jax.experimental import pallas as pl
from jax.experimental.pallas import tpu as pltpu
from jax.sharding import PartitionSpec as P


NORM_EPS = 1e-6
Z_COEF = 0.001
AUX_COEF = 0.01
GELU_C = 0.7978845608028654
GELU_K = 0.044715
BF = jnp.bfloat16
F32 = jnp.float32
TILE = 320
CHUNKS = 2
NT = (((1,), (1,)), ((), ()))
TN = (((0,), (0,)), ((), ()))


def widen_kernel(start_ref, x_ref, dy_ref, out_ref, wide):
    count = x_ref.shape[0]
    for j in range(4):
        lanes = slice(128 * j, 128 * (j + 1))
        wide[pl.ds(j, count, stride=8), :] = x_ref[:, lanes].astype(F32)
        wide[pl.ds(4 + j, count, stride=8), :] = dy_ref[:, lanes].astype(F32)
    out_ref[...] = wide[...].reshape(count, 8, 128).astype(BF)


def widen_rows(x, dy, start, count):
    block = 512
    width = x.shape[1]
    source = pl.BlockSpec((block, width), lambda i, first: (first[0] + i, 0))
    first = jnp.full((1,), start // block, jnp.int32)
    return pl.pallas_call(
        widen_kernel,
        grid_spec=pltpu.PrefetchScalarGridSpec(
            num_scalar_prefetch=1,
            grid=(count // block,),
            in_specs=[source, source],
            out_specs=pl.BlockSpec((block, 8, 128), lambda i, _: (i, 0, 0)),
            scratch_shapes=[pltpu.VMEM((block * 8, 128), F32)],
        ),
        out_shape=jax.ShapeDtypeStruct((count, 8, 128), BF),
        compiler_params=pltpu.CompilerParams(dimension_semantics=("arbitrary",), vmem_limit_bytes=60 * 1024 * 1024),
        cost_estimate=pl.CostEstimate(flops=count * 1_000_000, bytes_accessed=count * width * 8, transcendentals=0),
        name="widen_rows",
    )(first, x, dy)


def expert_kernel(n_piece, has_acc, has_prev, cap, idx_ref, *refs):
    pieces = refs[:n_piece]
    refs = refs[n_piece:]
    gate_ref, scale_ref, wg_ref, wl_ref, wo_ref = refs[:5]
    refs = refs[5:]
    acc_refs = refs[:3] if has_acc else None
    refs = refs[3:] if has_acc else refs
    refs = refs[2:] if has_prev else refs
    o_ref, du_ref, dg_ref, dl_ref, do_ref, table, rows, sems = refs
    step = pl.program_id(0)
    piece_rows = table.shape[0] // n_piece

    @pl.when(step == 0)
    def _():
        copies = [
            pltpu.make_async_copy(pieces[i], table.at[pl.ds(i * piece_rows, piece_rows)], sems.at[i])
            for i in range(n_piece)
        ]
        for c in copies:
            c.start()
        for c in copies:
            c.wait()

    base = step * cap

    def pick(i, _):
        for k in range(16):
            r = i * 16 + k
            rows[pl.ds(pl.multiple_of(r * 8, 8), 8), :] = table[idx_ref[base + r]].astype(F32)
        return 0

    lax.fori_loop(0, cap // 16, pick, 0)

    for out, i in ((dg_ref, 0), (dl_ref, 1), (do_ref, 2)):
        out[...] = acc_refs[i][...] if has_acc else jnp.zeros_like(out)

    wg, wl, wo = wg_ref[0], wl_ref[0], wo_ref[0]

    def tile(t, _):
        r0 = pl.multiple_of(t * TILE, TILE)

        def cols(j):
            return rows[pl.ds(r0 * 8 + j, TILE, stride=8), :]

        x = jnp.concatenate([cols(j) for j in range(4)], axis=1)
        gv = gate_ref[0, pl.ds(r0, TILE), :]
        inv = lax.rsqrt(jnp.mean(x * x, axis=-1, keepdims=True) + NORM_EPS)
        inv = jnp.where(gv[:, 1:2] > 0.0, inv, 0.0)
        u = (x * inv * scale_ref[...]).astype(BF)
        a0 = jnp.dot(u, wg, preferred_element_type=F32)
        a1 = jnp.dot(u, wl, preferred_element_type=F32)
        sq = a0 * a0
        th = jnp.tanh(GELU_C * a0 * (1.0 + GELU_K * sq))
        half = 0.5 * (1.0 + th)
        ge = a0 * half
        gp = half + 0.5 * a0 * (1.0 - th * th) * (GELU_C * (1.0 + 3.0 * GELU_K * sq))
        h = (ge * a1).astype(BF)
        o = jnp.dot(h, wo, preferred_element_type=F32).astype(BF)
        for k in range(4):
            o_ref[k, pl.ds(r0, TILE), :] = o[:, 128 * k:128 * (k + 1)]
        dy = jnp.concatenate([cols(4 + j) for j in range(4)], axis=1)
        d_o = (dy * gv[:, 0:1]).astype(BF)
        dh = lax.dot_general(d_o, wo, NT, preferred_element_type=F32)
        da0 = (dh * a1 * gp).astype(BF)
        da1 = (dh * ge).astype(BF)
        du = lax.dot_general(da0, wg, NT, preferred_element_type=F32)
        du = (du + lax.dot_general(da1, wl, NT, preferred_element_type=F32)).astype(BF)
        for k in range(4):
            du_ref[k, pl.ds(r0, TILE), :] = du[:, 128 * k:128 * (k + 1)]
        dg_ref[0] += lax.dot_general(u, da0, TN, preferred_element_type=F32)
        dl_ref[0] += lax.dot_general(u, da1, TN, preferred_element_type=F32)
        do_ref[0] += lax.dot_general(h, d_o, TN, preferred_element_type=F32)
        return 0

    lax.fori_loop(0, cap // TILE, tile, 0)


def run_experts(idx, pieces, gates, scale, wg, wl, wo, acc, prev):
    experts, cap, _ = gates.shape
    width, ff = wg.shape[1:]
    tokens = sum(p.shape[0] for p in pieces)
    n_piece = len(pieces)
    has_acc = acc is not None
    any_spec = pl.BlockSpec(memory_space=pl.ANY)
    by_exp = lambda *s: pl.BlockSpec((1,) + s, lambda e, _: (e, 0, 0))
    in_specs = [any_spec] * n_piece + [
        by_exp(cap, 2),
        pl.BlockSpec((1, width), lambda e, _: (0, 0)),
        by_exp(width, ff), by_exp(width, ff), by_exp(ff, width),
    ]
    args = list(pieces) + [gates, scale, wg, wl, wo]
    grad_specs = [by_exp(width, ff), by_exp(width, ff), by_exp(ff, width)]
    grad_shapes = [jax.ShapeDtypeStruct(w.shape, F32) for w in (wg, wl, wo)]
    aliases = {}
    if has_acc:
        for i in range(3):
            aliases[1 + len(args) + i] = 2 + i
        in_specs += grad_specs
        args += list(acc)
    lanes = width // 4
    shift = 0
    if prev is not None:
        for i in range(2):
            aliases[1 + len(args) + i] = i
        in_specs += [any_spec] * 2
        args += list(prev)
        shift = experts
    row_spec = pl.BlockSpec((4, cap, lanes), lambda e, _: (0, e + shift, 0))
    row_shape = jax.ShapeDtypeStruct((4, 2 * experts * cap, lanes), BF)
    flops = 2 * 9 * experts * cap * width * ff
    moved = tokens * width * 4 + experts * cap * width * 4 + 3 * width * ff * experts * (2 + 4 + 4 * has_acc)
    return pl.pallas_call(
        functools.partial(expert_kernel, n_piece, has_acc, prev is not None, cap),
        grid_spec=pltpu.PrefetchScalarGridSpec(
            num_scalar_prefetch=1,
            grid=(experts,),
            in_specs=in_specs,
            out_specs=[row_spec, row_spec] + grad_specs,
            scratch_shapes=[
                pltpu.VMEM((tokens, 8, 128), BF),
                pltpu.VMEM((cap * 8, 128), F32),
                pltpu.SemaphoreType.DMA((n_piece,)),
            ],
        ),
        out_shape=[row_shape, row_shape] + grad_shapes,
        input_output_aliases=aliases,
        compiler_params=pltpu.CompilerParams(
            dimension_semantics=("arbitrary",), vmem_limit_bytes=60 * 1024 * 1024),
        cost_estimate=pl.CostEstimate(flops=flops, bytes_accessed=moved, transcendentals=experts * cap * ff),
        name="experts_acc" if has_acc else "experts_new",
    )(idx, *args)


def collect_kernel(idx_ref, *refs):
    parts, refs = refs[:4], refs[4:]
    first_ref, second_ref, raw, table, sems = refs
    part_rows = parts[0].shape[0]
    copies = [
        pltpu.make_async_copy(parts[i], raw.at[pl.ds(i * part_rows, part_rows)], sems.at[i])
        for i in range(4)
    ]
    for c in copies:
        c.start()
    table[pl.ds(4 * part_rows, 8), :] = jnp.zeros((8, table.shape[1]), F32)
    for i in range(4):
        copies[i].wait()

        def widen(b, _):
            r = pl.multiple_of(i * part_rows + b * 128, 128)
            table[pl.ds(r, 128), :] = raw[pl.ds(r, 128), :].astype(F32)
            return 0

        lax.fori_loop(0, part_rows // 128, widen, 0)

    def pick(b, _):
        for k in range(8):
            t = b * 8 + k
            first_ref[pl.ds(t, 1), :] = table[pl.ds(idx_ref[0, t], 1), :]
            second_ref[pl.ds(t, 1), :] = table[pl.ds(idx_ref[1, t], 1), :]
        return 0

    lax.fori_loop(0, first_ref.shape[0] // 8, pick, 0)


def collect_rows(idx, parts):
    count = idx.shape[1]
    part_rows, lanes = parts[0].shape
    whole = pl.BlockSpec((count, lanes), lambda i, _: (0, 0))
    shape = jax.ShapeDtypeStruct((count, lanes), F32)
    return pl.pallas_call(
        collect_kernel,
        grid_spec=pltpu.PrefetchScalarGridSpec(
            num_scalar_prefetch=1,
            grid=(1,),
            in_specs=[pl.BlockSpec(memory_space=pl.ANY)] * 4,
            out_specs=[whole, whole],
            scratch_shapes=[
                pltpu.VMEM((4 * part_rows, lanes), BF),
                pltpu.VMEM((4 * part_rows + 8, lanes), F32),
                pltpu.SemaphoreType.DMA((4,)),
            ],
        ),
        out_shape=[shape, shape],
        compiler_params=pltpu.CompilerParams(
            dimension_semantics=("arbitrary",), vmem_limit_bytes=48 * 1024 * 1024),
        cost_estimate=pl.CostEstimate(flops=20_000_000_000, bytes_accessed=14_000_000, transcendentals=0),
        name="collect_rows",
    )(idx, *parts)


def choice_positions(idx_loc, experts):
    tok_count = idx_loc.shape[0]
    block = 128
    ids = jnp.arange(experts, dtype=jnp.int32)
    hit1 = idx_loc[:, 0:1] == ids
    hit2 = idx_loc[:, 1:2] == ids
    hits = jnp.concatenate([hit1, hit2], axis=1).astype(BF)
    blocks = hits.reshape(tok_count // block, block, 2 * experts)
    tri = (jnp.arange(block)[:, None] > jnp.arange(block)[None, :]).astype(BF)
    inner = jnp.einsum('ij,bjk->bik', tri, blocks, preferred_element_type=F32)
    sums = jnp.sum(blocks.astype(F32), axis=1)
    outer = jnp.cumsum(sums, axis=0) - sums
    count = jnp.sum(sums, axis=0)
    outer = outer + jnp.concatenate([jnp.zeros_like(count[:experts]), count[:experts]])
    rank = (inner + outer[:, None, :]).reshape(tok_count, 2 * experts)
    rank = rank * hits.astype(F32)
    pos1 = jnp.sum(rank[:, :experts], axis=1).astype(jnp.int32)
    pos2 = jnp.sum(rank[:, experts:], axis=1).astype(jnp.int32)
    return hit1, hit2, pos1, pos2, count[:experts]


def split3(v):
    hi = v.astype(BF)
    rest = v - hi.astype(F32)
    mid = rest.astype(BF)
    return hi, mid, (rest - mid.astype(F32)).astype(BF)


def slot_table(hit1, hit2, pos1, pos2, g1, g2, cap):
    tok_count, experts = hit1.shape
    tok = jnp.arange(1, tok_count + 1, dtype=jnp.int32)
    hi = (tok // 128).astype(BF)
    lo = (tok % 128).astype(BF)
    slots = jnp.arange(cap, dtype=jnp.int32)
    total = 0.0
    for hit, pos, g in ((hit1, pos1, g1), (hit2, pos2, g2)):
        vals = (hi, lo) + split3(g)
        left = jnp.concatenate([jnp.where(hit, v[:, None], BF(0)) for v in vals], axis=1)
        at = (pos[:, None] == slots).astype(BF)
        total = total + jnp.einsum('tk,tc->kc', left, at, preferred_element_type=F32)
    total = total.reshape(5, experts, cap)
    tok1 = total[0] * 128.0 + total[1]
    gate = (total[2] + total[3]) + total[4]
    return tok1, gate


def solution(mesh):
    ep_size = mesh.shape['ep']
    tp_size = mesh.shape['tp']

    def swap(v, bit):
        return lax.ppermute(v, 'ep', [(i, i ^ bit) for i in range(ep_size)])

    def device_block(x_loc, dy_loc, idx_loc, norm_scale, w_router, gate_loc, lin_loc, out_loc):
        tok_count, width = x_loc.shape
        experts = w_router.shape[1]
        local_exp = gate_loc.shape[0]
        tokens = tok_count * ep_size
        slot_cap = (5 * tok_count + 2 * experts - 1) // (2 * experts)
        ep_idx = lax.axis_index('ep')
        tp_idx = lax.axis_index('tp')
        quarter = tok_count // tp_size
        lanes = width // tp_size

        q_start = tp_idx * quarter
        part = quarter // CHUNKS
        sent, cuts = [], []
        for c in range(CHUNKS):
            rows = widen_rows(x_loc, dy_loc, q_start + c * part, part)
            cuts.append(rows)
            sent.append(swap(rows, 2))
        x_own, dy_own, _ = lax.optimization_barrier((x_loc, dy_loc, cuts))
        own = widen_rows(x_own, dy_own, 0, tok_count)
        partner = swap(own, 1)
        far = []
        for c in range(CHUNKS):
            far.append(lax.all_gather(sent[c], 'tp', tiled=True))
        far_partner = [swap(f, 1) for f in far]

        x_wide = x_loc.astype(F32)
        inv_rms = lax.rsqrt(jnp.mean(x_wide * x_wide, axis=-1, keepdims=True) + NORM_EPS)
        x_norm = x_wide * inv_rms
        u_tok = (x_norm * norm_scale).astype(BF)
        u_wide = u_tok.astype(F32)
        logits = jnp.dot(u_wide, w_router, preferred_element_type=F32)
        log_norm = jax.nn.logsumexp(logits, axis=-1)
        router_prob = jnp.exp(logits - log_norm[:, None])
        hit1, hit2, pos1, pos2, count_loc = choice_positions(idx_loc, experts)
        one_first = hit1.astype(F32)
        one_second = hit2.astype(F32)
        stats = jnp.concatenate([count_loc, jnp.sum(router_prob, axis=0), jnp.sum(log_norm * log_norm)[None]])
        gate_first = jnp.sum(router_prob * one_first, axis=-1)
        gate_second = jnp.sum(router_prob * one_second, axis=-1)
        gate_total = gate_first + gate_second
        norm_first = gate_first / gate_total
        norm_second = gate_second / gate_total

        tok1, slot_gate = slot_table(hit1, hit2, pos1, pos2, norm_first, norm_second, slot_cap)
        info = jnp.stack([tok1, slot_gate], axis=1)
        info = lax.all_to_all(info, 'ep', 0, 0, tiled=True).reshape(ep_size, local_exp, 2, slot_cap)

        scale_row = norm_scale[None, :]
        acc = None
        pairs = []
        for rel, pieces in enumerate(([own], [partner], far, far_partner)):
            mine = lax.dynamic_index_in_dim(info, ep_idx ^ rel, 0, keepdims=False)
            tok = mine[:, 0].astype(jnp.int32)
            valid = (tok > 0).astype(F32)
            tok = jnp.maximum(tok - 1, 0)
            if len(pieces) > 1:
                q, rest = tok // quarter, tok % quarter
                tok = (rest // part) * (tp_size * part) + q * part + rest % part
            gates = jnp.stack([mine[:, 1], valid], axis=-1)
            prev = (o, du) if rel % 2 else None
            o, du, *acc = run_experts(tok.reshape(-1), pieces, gates, scale_row, gate_loc, lin_loc, out_loc, acc, prev)
            if rel % 2:
                pairs.append((o, du))
        d_gate, d_lin, d_out = acc
        (o_near, du_near), (o_far, du_far) = pairs
        stats, o_far = lax.optimization_barrier((stats, o_far))
        stats = lax.psum(stats, 'ep')
        frac_first = stats[:experts] / tokens
        z_loss = Z_COEF * stats[2 * experts] / tokens
        aux_loss = AUX_COEF * experts * jnp.sum(frac_first * stats[experts:2 * experts]) / tokens

        def scatter_sum(v):
            flat = v.reshape(-1, v.shape[2])
            return lax.optimization_barrier(lax.psum_scatter(flat, 'tp', scatter_dimension=0, tiled=True))

        def spread(near, far):
            half = near.shape[0] // 2
            return [near[:half], swap(near[half:], 1), swap(far[:half], 2), swap(far[half:], 3)]

        o_near = scatter_sum(o_near)
        o_far = scatter_sum(o_far)
        du_far = scatter_sum(du_far)
        du_near = scatter_sum(du_near)

        def place(ids, pos):
            rel = (ids // local_exp) ^ ep_idx
            slot = (rel * local_exp + ids % local_exp) * slot_cap + pos
            return jnp.where(pos < slot_cap, slot, experts * slot_cap)

        both = jnp.stack([place(idx_loc[:, 0], pos1), place(idx_loc[:, 1], pos2)])

        def fetch(parts):
            return collect_rows(both, parts)

        c_start = tp_idx * lanes
        col = lambda v: lax.dynamic_slice_in_dim(v, c_start, lanes, axis=v.ndim - 1)
        x_col = col(x_loc).astype(F32)
        dy_col = col(dy_loc).astype(F32)
        xn_col = x_col * inv_rms
        scale_col = col(norm_scale)
        u_col = (xn_col * scale_col).astype(BF).astype(F32)
        wr_col = lax.dynamic_slice_in_dim(w_router, c_start, lanes, axis=0)

        o1, o2 = fetch(spread(o_near, o_far))
        y_col = (x_col + norm_first[:, None] * o1 + norm_second[:, None] * o2).astype(BF)
        dn1 = jnp.sum(dy_col * o1, axis=-1)
        dn2 = jnp.sum(dy_col * o2, axis=-1)
        dn_first = lax.psum(dn1, 'tp')
        dn2, dn_first = lax.optimization_barrier((dn2, dn_first))
        dn_second = lax.psum(dn2, 'tp')
        gate_mix = norm_first * dn_first + norm_second * dn_second
        y_col, du_near = lax.optimization_barrier((y_col, du_near))
        aux_coef = AUX_COEF * experts * frac_first
        d_logits = router_prob * (aux_coef - jnp.sum(aux_coef * router_prob, axis=-1, keepdims=True))
        d_logits = d_logits + (2.0 * Z_COEF) * log_norm[:, None] * router_prob
        d_logits = d_logits + one_first * (norm_first * (dn_first - gate_mix))[:, None]
        d_logits = d_logits + one_second * (norm_second * (dn_second - gate_mix))[:, None]
        d_router_col = jnp.einsum('td,te->de', u_col, d_logits, preferred_element_type=F32)
        du_dense = jnp.einsum('te,de->td', d_logits, wr_col, preferred_element_type=F32)

        du1, du2 = fetch(spread(du_near, du_far))
        du_all = du1 + du2 + du_dense
        d_scale_col = jnp.sum(du_all * xn_col, axis=0)
        dxn = du_all * scale_col
        proj = lax.psum(jnp.sum(dxn * xn_col, axis=-1), 'tp')[:, None] / width
        dx_col = (dy_col + inv_rms * (dxn - xn_col * proj)).astype(BF)

        def full(v):
            return lax.all_gather(v, 'tp', axis=1, tiled=True)

        y_loc = full(y_col)
        dx_loc = full(dx_col)
        d_router = lax.all_gather(lax.psum(d_router_col, 'ep'), 'tp', axis=0, tiled=True)
        d_scale = lax.all_gather(lax.psum(d_scale_col, 'ep'), 'tp', axis=0, tiled=True)
        losses = jnp.stack([z_loss, aux_loss])
        return (y_loc, losses, dx_loc, d_scale, d_router, d_gate, d_lin, d_out)

    tok_spec = P('ep', None)
    in_spec = P('ep', None, 'tp')
    out_spec = P('ep', 'tp', None)
    return jax.shard_map(device_block, mesh=mesh, in_specs=(tok_spec, tok_spec, tok_spec, P(), P(), in_spec, in_spec, out_spec), out_specs=(tok_spec, P(), tok_spec, P(), P(), in_spec, in_spec, out_spec), check_vma=False)
```

```python
import functools

import jax
import jax.numpy as jnp
from jax import lax
from jax.experimental import pallas as pl
from jax.experimental.pallas import tpu as pltpu
from jax.sharding import PartitionSpec as P


NORM_EPS = 1e-6
Z_COEF = 0.001
AUX_COEF = 0.01
GELU_C = 0.7978845608028654
GELU_K = 0.044715
BF = jnp.bfloat16
F32 = jnp.float32
TILE = 640
CHUNKS = (3, 5)
NT = (((1,), (1,)), ((), ()))
TN = (((0,), (0,)), ((), ()))


def widen_kernel(start_ref, x_ref, dy_ref, out_ref, wide):
    count = x_ref.shape[0]
    for j in range(4):
        lanes = slice(128 * j, 128 * (j + 1))
        wide[pl.ds(j, count, stride=8), :] = x_ref[:, lanes].astype(F32)
        wide[pl.ds(4 + j, count, stride=8), :] = dy_ref[:, lanes].astype(F32)
    out_ref[...] = wide[...].reshape(count, 8, 128).astype(BF)


def widen_rows(x, dy, start, count):
    block = 256
    width = x.shape[1]
    source = pl.BlockSpec((block, width), lambda i, first: (first[0] + i, 0))
    first = jnp.full((1,), start // block, jnp.int32)
    return pl.pallas_call(
        widen_kernel,
        grid_spec=pltpu.PrefetchScalarGridSpec(
            num_scalar_prefetch=1,
            grid=(count // block,),
            in_specs=[source, source],
            out_specs=pl.BlockSpec((block, 8, 128), lambda i, _: (i, 0, 0)),
            scratch_shapes=[pltpu.VMEM((block * 8, 128), F32)],
        ),
        out_shape=jax.ShapeDtypeStruct((count, 8, 128), BF),
        compiler_params=pltpu.CompilerParams(dimension_semantics=("arbitrary",), vmem_limit_bytes=60 * 1024 * 1024),
        cost_estimate=pl.CostEstimate(flops=count * 1_000_000, bytes_accessed=count * width * 8, transcendentals=0),
        name="widen_rows",
    )(first, x, dy)


def expert_kernel(n_piece, has_acc, has_prev, cap, idx_ref, *refs):
    pieces = refs[:n_piece]
    refs = refs[n_piece:]
    gate_ref, scale_ref, wg_ref, wl_ref, wo_ref = refs[:5]
    refs = refs[5:]
    acc_refs = refs[:3] if has_acc else None
    refs = refs[3:] if has_acc else refs
    refs = refs[2:] if has_prev else refs
    o_ref, du_ref, dg_ref, dl_ref, do_ref, table, rows, u_all, h_all, dy_all, a0_all, a1_all, sems = refs
    step = pl.program_id(0)
    starts = [sum(p.shape[0] for p in pieces[:i]) for i in range(n_piece)]

    def pick(base, r):
        rows[pl.ds(pl.multiple_of(r * 8, 8), 8), :] = table[idx_ref[base + r]].astype(F32)

    @pl.when(step == 0)
    def _():
        copies = [
            pltpu.make_async_copy(pieces[i], table.at[pl.ds(starts[i], pieces[i].shape[0])], sems.at[i])
            for i in range(n_piece)
        ]
        for c in copies:
            c.start()
        for c in copies:
            c.wait()

        def some(i, _):
            for k in range(16):
                pick(0, i * 16 + k)
            return 0

        lax.fori_loop(0, cap // 16, some, 0)

    later = jnp.minimum(step + 1, pl.num_programs(0) - 1) * cap
    wg, wl, wo = wg_ref[0], wl_ref[0], wo_ref[0]

    def tile(t, _):
        r0 = pl.multiple_of(t * TILE, TILE)
        here = pl.ds(r0, TILE)

        def cols(j):
            return rows[pl.ds(r0 * 8 + j, TILE, stride=8), :]

        x = jnp.concatenate([cols(j) for j in range(4)], axis=1)
        dy = jnp.concatenate([cols(4 + j) for j in range(4)], axis=1)
        gv = gate_ref[0, here, :]
        inv = lax.rsqrt(jnp.mean(x * x, axis=-1, keepdims=True) + NORM_EPS)
        inv = jnp.where(gv[:, 1:2] > 0.0, inv, 0.0)
        u = (x * inv * scale_ref[...]).astype(BF)
        d_o = (dy * gv[:, 0:1]).astype(BF)
        u_all[here, :] = u
        dy_all[here, :] = d_o
        for k in range(TILE):
            pick(later, r0 + k)
        a0 = jnp.dot(u, wg, preferred_element_type=F32)
        a1 = jnp.dot(u, wl, preferred_element_type=F32)
        dh = lax.dot_general(d_o, wo, NT, preferred_element_type=F32)
        sq = a0 * a0
        th = jnp.tanh(GELU_C * a0 * (1.0 + GELU_K * sq))
        half = 0.5 * (1.0 + th)
        ge = a0 * half
        gp = half + 0.5 * a0 * (1.0 - th * th) * (GELU_C * (1.0 + 3.0 * GELU_K * sq))
        h = (ge * a1).astype(BF)
        h_all[here, :] = h
        da0 = (dh * a1 * gp).astype(BF)
        da1 = (dh * ge).astype(BF)
        a0_all[here, :] = da0
        a1_all[here, :] = da1
        o = jnp.dot(h, wo, preferred_element_type=F32).astype(BF)
        for k in range(4):
            o_ref[k, here, :] = o[:, 128 * k:128 * (k + 1)]
        du = lax.dot_general(da0, wg, NT, preferred_element_type=F32)
        du = (du + lax.dot_general(da1, wl, NT, preferred_element_type=F32)).astype(BF)
        for k in range(4):
            du_ref[k, here, :] = du[:, 128 * k:128 * (k + 1)]
        return 0

    lax.fori_loop(0, cap // TILE, tile, 0)

    for i, (out, left, right) in enumerate(((dg_ref, u_all, a0_all), (dl_ref, u_all, a1_all), (do_ref, h_all, dy_all))):
        grad = lax.dot_general(left[...], right[...], TN, preferred_element_type=F32)
        out[0] = acc_refs[i][0] + grad if has_acc else grad


def run_experts(idx, pieces, gates, scale, wg, wl, wo, acc, prev):
    experts, cap, _ = gates.shape
    width, ff = wg.shape[1:]
    tokens = sum(p.shape[0] for p in pieces)
    n_piece = len(pieces)
    has_acc = acc is not None
    any_spec = pl.BlockSpec(memory_space=pl.ANY)
    by_exp = lambda *s: pl.BlockSpec((1,) + s, lambda e, _: (e, 0, 0))
    in_specs = [any_spec] * n_piece + [
        by_exp(cap, 2),
        pl.BlockSpec((1, width), lambda e, _: (0, 0)),
        by_exp(width, ff), by_exp(width, ff), by_exp(ff, width),
    ]
    args = list(pieces) + [gates, scale, wg, wl, wo]
    grad_specs = [by_exp(width, ff), by_exp(width, ff), by_exp(ff, width)]
    grad_shapes = [jax.ShapeDtypeStruct(w.shape, F32) for w in (wg, wl, wo)]
    aliases = {}
    if has_acc:
        for i in range(3):
            aliases[1 + len(args) + i] = 2 + i
        in_specs += grad_specs
        args += list(acc)
    lanes = width // 4
    shift = 0
    if prev is not None:
        for i in range(2):
            aliases[1 + len(args) + i] = i
        in_specs += [any_spec] * 2
        args += list(prev)
        shift = experts
    row_spec = pl.BlockSpec((4, cap, lanes), lambda e, _: (0, e + shift, 0))
    row_shape = jax.ShapeDtypeStruct((4, 2 * experts * cap, lanes), BF)
    flops = 2 * 9 * experts * cap * width * ff
    moved = tokens * width * 4 + experts * cap * width * 4 + 3 * width * ff * experts * (2 + 4 + 4 * has_acc)
    return pl.pallas_call(
        functools.partial(expert_kernel, n_piece, has_acc, prev is not None, cap),
        grid_spec=pltpu.PrefetchScalarGridSpec(
            num_scalar_prefetch=1,
            grid=(experts,),
            in_specs=in_specs,
            out_specs=[row_spec, row_spec] + grad_specs,
            scratch_shapes=[
                pltpu.VMEM((tokens, 8, 128), BF),
                pltpu.VMEM((cap * 8, 128), F32),
                pltpu.VMEM((cap, width), BF),
                pltpu.VMEM((cap, ff), BF),
                pltpu.VMEM((cap, width), BF),
                pltpu.VMEM((cap, ff), BF),
                pltpu.VMEM((cap, ff), BF),
                pltpu.SemaphoreType.DMA((n_piece,)),
            ],
        ),
        out_shape=[row_shape, row_shape] + grad_shapes,
        input_output_aliases=aliases,
        compiler_params=pltpu.CompilerParams(
            dimension_semantics=("arbitrary",), vmem_limit_bytes=60 * 1024 * 1024),
        cost_estimate=pl.CostEstimate(flops=flops, bytes_accessed=moved, transcendentals=experts * cap * ff),
        name="experts_acc" if has_acc else "experts_new",
    )(idx, *args)


def collect_kernel(idx_ref, *refs):
    parts, refs = refs[:4], refs[4:]
    first_ref, second_ref, raw, table, sems = refs
    part_rows = parts[0].shape[0]
    copies = [
        pltpu.make_async_copy(parts[i], raw.at[pl.ds(i * part_rows, part_rows)], sems.at[i])
        for i in range(4)
    ]
    for c in copies:
        c.start()
    table[pl.ds(4 * part_rows, 8), :] = jnp.zeros((8, table.shape[1]), F32)
    for i in range(4):
        copies[i].wait()

        def widen(b, _):
            r = pl.multiple_of(i * part_rows + b * 128, 128)
            table[pl.ds(r, 128), :] = raw[pl.ds(r, 128), :].astype(F32)
            return 0

        lax.fori_loop(0, part_rows // 128, widen, 0)

    def pick(b, _):
        for k in range(8):
            t = b * 8 + k
            first_ref[pl.ds(t, 1), :] = table[pl.ds(idx_ref[0, t], 1), :]
            second_ref[pl.ds(t, 1), :] = table[pl.ds(idx_ref[1, t], 1), :]
        return 0

    lax.fori_loop(0, first_ref.shape[0] // 8, pick, 0)


def collect_rows(idx, parts):
    count = idx.shape[1]
    part_rows, lanes = parts[0].shape
    whole = pl.BlockSpec((count, lanes), lambda i, _: (0, 0))
    shape = jax.ShapeDtypeStruct((count, lanes), F32)
    return pl.pallas_call(
        collect_kernel,
        grid_spec=pltpu.PrefetchScalarGridSpec(
            num_scalar_prefetch=1,
            grid=(1,),
            in_specs=[pl.BlockSpec(memory_space=pl.ANY)] * 4,
            out_specs=[whole, whole],
            scratch_shapes=[
                pltpu.VMEM((4 * part_rows, lanes), BF),
                pltpu.VMEM((4 * part_rows + 8, lanes), F32),
                pltpu.SemaphoreType.DMA((4,)),
            ],
        ),
        out_shape=[shape, shape],
        compiler_params=pltpu.CompilerParams(
            dimension_semantics=("arbitrary",), vmem_limit_bytes=48 * 1024 * 1024),
        cost_estimate=pl.CostEstimate(flops=20_000_000_000, bytes_accessed=14_000_000, transcendentals=0),
        name="collect_rows",
    )(idx, *parts)


def choice_positions(idx_loc, experts):
    tok_count = idx_loc.shape[0]
    block = 128
    ids = jnp.arange(experts, dtype=jnp.int32)
    hit1 = idx_loc[:, 0:1] == ids
    hit2 = idx_loc[:, 1:2] == ids
    hits = jnp.concatenate([hit1, hit2], axis=1).astype(BF)
    blocks = hits.reshape(tok_count // block, block, 2 * experts)
    tri = (jnp.arange(block)[:, None] > jnp.arange(block)[None, :]).astype(BF)
    inner = jnp.einsum('ij,bjk->bik', tri, blocks, preferred_element_type=F32)
    sums = jnp.sum(blocks.astype(F32), axis=1)
    outer = jnp.cumsum(sums, axis=0) - sums
    count = jnp.sum(sums, axis=0)
    outer = outer + jnp.concatenate([jnp.zeros_like(count[:experts]), count[:experts]])
    rank = (inner + outer[:, None, :]).reshape(tok_count, 2 * experts)
    rank = rank * hits.astype(F32)
    pos1 = jnp.sum(rank[:, :experts], axis=1).astype(jnp.int32)
    pos2 = jnp.sum(rank[:, experts:], axis=1).astype(jnp.int32)
    return hit1, hit2, pos1, pos2, count[:experts]


def split3(v):
    hi = v.astype(BF)
    rest = v - hi.astype(F32)
    mid = rest.astype(BF)
    return hi, mid, (rest - mid.astype(F32)).astype(BF)


def slot_table(hit1, hit2, pos1, pos2, g1, g2, cap):
    tok_count, experts = hit1.shape
    tok = jnp.arange(1, tok_count + 1, dtype=jnp.int32)
    hi = (tok // 128).astype(BF)
    lo = (tok % 128).astype(BF)
    slots = jnp.arange(cap, dtype=jnp.int32)
    total = 0.0
    for hit, pos, g in ((hit1, pos1, g1), (hit2, pos2, g2)):
        vals = (hi, lo) + split3(g)
        left = jnp.concatenate([jnp.where(hit, v[:, None], BF(0)) for v in vals], axis=1)
        at = (pos[:, None] == slots).astype(BF)
        total = total + jnp.einsum('tk,tc->kc', left, at, preferred_element_type=F32)
    total = total.reshape(5, experts, cap)
    tok1 = total[0] * 128.0 + total[1]
    gate = (total[2] + total[3]) + total[4]
    return tok1, gate


def solution(mesh):
    ep_size = mesh.shape['ep']
    tp_size = mesh.shape['tp']

    def swap(v, bit):
        return lax.ppermute(v, 'ep', [(i, i ^ bit) for i in range(ep_size)])

    def device_block(x_loc, dy_loc, idx_loc, norm_scale, w_router, gate_loc, lin_loc, out_loc):
        tok_count, width = x_loc.shape
        experts = w_router.shape[1]
        local_exp = gate_loc.shape[0]
        tokens = tok_count * ep_size
        slot_cap = (5 * tok_count + 2 * experts - 1) // (2 * experts)
        ep_idx = lax.axis_index('ep')
        tp_idx = lax.axis_index('tp')
        quarter = tok_count // tp_size
        lanes = width // tp_size

        q_start = tp_idx * quarter
        parts = [quarter * c // sum(CHUNKS) for c in CHUNKS]
        sent, cuts = [], []
        for c, part in enumerate(parts):
            rows = widen_rows(x_loc, dy_loc, q_start + sum(parts[:c]), part)
            cuts.append(rows)
            sent.append(swap(rows, 2))
        x_own, dy_own, _ = lax.optimization_barrier((x_loc, dy_loc, cuts))
        own = widen_rows(x_own, dy_own, 0, tok_count)
        partner = swap(own, 1)
        far = []
        for c in range(len(parts)):
            far.append(lax.all_gather(sent[c], 'tp', tiled=True))
        far_partner = [swap(f, 1) for f in far]

        x_wide = x_loc.astype(F32)
        inv_rms = lax.rsqrt(jnp.mean(x_wide * x_wide, axis=-1, keepdims=True) + NORM_EPS)
        x_norm = x_wide * inv_rms
        u_tok = (x_norm * norm_scale).astype(BF)
        u_wide = u_tok.astype(F32)
        logits = jnp.dot(u_wide, w_router, preferred_element_type=F32)
        log_norm = jax.nn.logsumexp(logits, axis=-1)
        router_prob = jnp.exp(logits - log_norm[:, None])
        hit1, hit2, pos1, pos2, count_loc = choice_positions(idx_loc, experts)
        one_first = hit1.astype(F32)
        one_second = hit2.astype(F32)
        stats = jnp.concatenate([count_loc, jnp.sum(router_prob, axis=0), jnp.sum(log_norm * log_norm)[None]])
        gate_first = jnp.sum(router_prob * one_first, axis=-1)
        gate_second = jnp.sum(router_prob * one_second, axis=-1)
        gate_total = gate_first + gate_second
        norm_first = gate_first / gate_total
        norm_second = gate_second / gate_total

        tok1, slot_gate = slot_table(hit1, hit2, pos1, pos2, norm_first, norm_second, slot_cap)
        info = jnp.stack([tok1, slot_gate], axis=1)
        info = lax.all_to_all(info, 'ep', 0, 0, tiled=True).reshape(ep_size, local_exp, 2, slot_cap)

        scale_row = norm_scale[None, :]
        acc = None
        pairs = []
        for rel, pieces in enumerate(([own], [partner], far, far_partner)):
            mine = lax.dynamic_index_in_dim(info, ep_idx ^ rel, 0, keepdims=False)
            tok = mine[:, 0].astype(jnp.int32)
            valid = (tok > 0).astype(F32)
            tok = jnp.maximum(tok - 1, 0)
            if len(pieces) > 1:
                q, rest = tok // quarter, tok % quarter
                tok = jnp.where(
                    rest < parts[0], q * parts[0] + rest,
                    tp_size * parts[0] + q * parts[1] + rest - parts[0])
            gates = jnp.stack([mine[:, 1], valid], axis=-1)
            prev = (o, du) if rel % 2 else None
            o, du, *acc = run_experts(tok.reshape(-1), pieces, gates, scale_row, gate_loc, lin_loc, out_loc, acc, prev)
            if rel % 2:
                pairs.append((o, du))
        d_gate, d_lin, d_out = acc
        (o_near, du_near), (o_far, du_far) = pairs
        stats, o_far = lax.optimization_barrier((stats, o_far))
        stats = lax.psum(stats, 'ep')
        frac_first = stats[:experts] / tokens
        z_loss = Z_COEF * stats[2 * experts] / tokens
        aux_loss = AUX_COEF * experts * jnp.sum(frac_first * stats[experts:2 * experts]) / tokens

        def scatter_sum(v):
            flat = v.reshape(-1, v.shape[2])
            return lax.optimization_barrier(lax.psum_scatter(flat, 'tp', scatter_dimension=0, tiled=True))

        def spread(near, far):
            half = near.shape[0] // 2
            return [near[:half], swap(near[half:], 1), swap(far[:half], 2), swap(far[half:], 3)]

        o_near = scatter_sum(o_near)
        o_far = scatter_sum(o_far)
        du_far = scatter_sum(du_far)
        du_near = scatter_sum(du_near)

        def place(ids, pos):
            rel = (ids // local_exp) ^ ep_idx
            slot = (rel * local_exp + ids % local_exp) * slot_cap + pos
            return jnp.where(pos < slot_cap, slot, experts * slot_cap)

        both = jnp.stack([place(idx_loc[:, 0], pos1), place(idx_loc[:, 1], pos2)])

        def fetch(parts):
            return collect_rows(both, parts)

        c_start = tp_idx * lanes
        col = lambda v: lax.dynamic_slice_in_dim(v, c_start, lanes, axis=v.ndim - 1)
        x_col = col(x_loc).astype(F32)
        dy_col = col(dy_loc).astype(F32)
        xn_col = x_col * inv_rms
        scale_col = col(norm_scale)
        u_col = (xn_col * scale_col).astype(BF).astype(F32)
        wr_col = lax.dynamic_slice_in_dim(w_router, c_start, lanes, axis=0)

        o1, o2 = fetch(spread(o_near, o_far))
        y_col = (x_col + norm_first[:, None] * o1 + norm_second[:, None] * o2).astype(BF)
        dn1 = jnp.sum(dy_col * o1, axis=-1)
        dn2 = jnp.sum(dy_col * o2, axis=-1)
        dn_first = lax.psum(dn1, 'tp')
        dn2, dn_first = lax.optimization_barrier((dn2, dn_first))
        dn_second = lax.psum(dn2, 'tp')
        gate_mix = norm_first * dn_first + norm_second * dn_second
        y_col, du_near = lax.optimization_barrier((y_col, du_near))
        aux_coef = AUX_COEF * experts * frac_first
        d_logits = router_prob * (aux_coef - jnp.sum(aux_coef * router_prob, axis=-1, keepdims=True))
        d_logits = d_logits + (2.0 * Z_COEF) * log_norm[:, None] * router_prob
        d_logits = d_logits + one_first * (norm_first * (dn_first - gate_mix))[:, None]
        d_logits = d_logits + one_second * (norm_second * (dn_second - gate_mix))[:, None]
        d_router_col = jnp.einsum('td,te->de', u_col, d_logits, preferred_element_type=F32)
        du_dense = jnp.einsum('te,de->td', d_logits, wr_col, preferred_element_type=F32)

        du1, du2 = fetch(spread(du_near, du_far))
        du_all = du1 + du2 + du_dense
        d_scale_col = jnp.sum(du_all * xn_col, axis=0)
        dxn = du_all * scale_col
        proj = lax.psum(jnp.sum(dxn * xn_col, axis=-1), 'tp')[:, None] / width
        dx_col = (dy_col + inv_rms * (dxn - xn_col * proj)).astype(BF)

        def full(v):
            return lax.all_gather(v, 'tp')

        def join(v):
            return v.transpose(1, 0, 2).reshape(tok_count, width)

        y_loc = join(full(y_col))
        dx_loc = join(full(dx_col))
        d_router = lax.all_gather(lax.psum(d_router_col, 'ep'), 'tp', axis=0, tiled=True)
        d_scale = lax.all_gather(lax.psum(d_scale_col, 'ep'), 'tp', axis=0, tiled=True)
        losses = jnp.stack([z_loss, aux_loss])
        return (y_loc, losses, dx_loc, d_scale, d_router, d_gate, d_lin, d_out)

    tok_spec = P('ep', None)
    in_spec = P('ep', None, 'tp')
    out_spec = P('ep', 'tp', None)
    return jax.shard_map(device_block, mesh=mesh, in_specs=(tok_spec, tok_spec, tok_spec, P(), P(), in_spec, in_spec, out_spec), out_specs=(tok_spec, P(), tok_spec, P(), P(), in_spec, in_spec, out_spec), check_vma=False)
```
